32 devices in a mesh: dp: 8 (over z, x), cent: 4 (over y, core).
Axes of the slice: x: 2, y: 2, z: 4, core: 2. Of those that a mesh axis runs over, the one named last changes fastest.
Arguments:
- documents: bfloat16 [16384, 2048], P(('dp', 'cent')), may hold values from -6 to 6
- assigned: int32 [16384], P(('dp', 'cent')), may hold values from 0 to 12287, as said below
- centroids: bfloat16 [12288, 2048], P(('dp', 'cent')), may hold values from -6 to 6
- owner_slot: int32 [12288], replicated, may hold values from 0 to 12287, as said below
Outputs:
- prototypicality: float32 [16384], P(('dp', 'cent'))
- redundancy: float32 [16384], P(('dp', 'cent'))
- cluster_stats: float32 [3, 12288], P(None, ('dp', 'cent'))
The draws below stay inside these ranges and needn't reach their ends.
Inputs may be any that keep to these rules, and one draw needn't show every extreme that they name: `owner_slot`: A permutation of the cluster numbers. `assigned`: of the 512 documents of one device, at most 32 have a slot in any one owner's block of 384 slots, and at most 80 have slots with the owners that share one dp index; in every draw some device reaches 80, and one owner receives exactly 32 from every device.
All inputs are finite; a program needn't handle non-finite values.
Results may differ from the reference program's by a relative error of at most 0.0003.
Values may be sent and summed in bfloat16 or wider, within the bound.
A program may use at most 64 MiB of HBM per device.

```python
import jax
import jax.numpy as jnp
from jax import lax

D = 2048
DOC_DEV = 512
CL_DEV = 384
DOCS = 16384
CLUSTERS = 12288
CAP = 32
GCAP = 80
N_CENT = 4
DEVICES = 32


def slot_permutation(key):
    return jax.random.permutation(jax.random.fold_in(key, 11), CLUSTERS).astype(jnp.int32)


def draw_owner_slot(key, part):
    return slot_permutation(key)


def draw_assigned(key, part):
    permuted = slot_permutation(key)
    inverse = jnp.zeros((CLUSTERS,), jnp.int32).at[permuted].set(jnp.arange(CLUSTERS, dtype=jnp.int32))
    base = jax.random.fold_in(key, 23)
    key_forced = jax.random.fold_in(base, 1)
    key_favour = jax.random.fold_in(base, 2)
    key_ticket = jax.random.fold_in(base, 3)
    key_choose = jax.random.fold_in(base, 4)
    key_shuffle = jax.random.fold_in(base, 5)
    key_local = jax.random.fold_in(base, 6)
    row_count = DEVICES // N_CENT
    per_row = N_CENT * CAP
    forced = jax.random.randint(key_forced, (), 0, DEVICES, dtype=jnp.int32)
    forced_row = forced // N_CENT
    forced_col = forced % N_CENT
    row_ids = jnp.arange(row_count, dtype=jnp.int32)[None, :]
    favour = jax.random.randint(key_favour, (DEVICES, row_count), 0, N_CENT, dtype=jnp.int32)
    favour = jnp.where(row_ids == forced_row, forced_col, favour)
    ticket_ids = jnp.arange(per_row, dtype=jnp.int32)
    ticket_col = ticket_ids // CAP
    noise = jax.random.randint(key_ticket, (DEVICES, row_count, per_row), 0, 1 << 19, dtype=jnp.int32)
    boost = jnp.where(ticket_col[None, None, :] == favour[:, :, None], 1 << 29, 0).astype(jnp.int32)
    score = noise * per_row + ticket_ids[None, None, :] + boost
    kept = jnp.argsort(-score, axis=-1)[:, :, :GCAP].astype(jnp.int32)
    kept_owner = row_ids[:, :, None] * N_CENT + kept // CAP
    kept_owner = kept_owner.reshape(DEVICES, row_count * GCAP)
    pool = row_count * GCAP
    pool_ids = jnp.arange(pool, dtype=jnp.int32)
    pool_row = pool_ids // GCAP
    noise_two = jax.random.randint(key_choose, (DEVICES, pool), 0, 1 << 19, dtype=jnp.int32)
    boost_two = jnp.where(pool_row == forced_row, 1 << 29, 0).astype(jnp.int32)
    score_two = noise_two * pool + pool_ids[None, :] + boost_two[None, :]
    chosen = jnp.argsort(-score_two, axis=-1)[:, :DOC_DEV].astype(jnp.int32)
    chosen_owner = jnp.take_along_axis(kept_owner, chosen, axis=1)
    noise_three = jax.random.randint(key_shuffle, (DEVICES, DOC_DEV), 0, 1 << 19, dtype=jnp.int32)
    score_three = noise_three * DOC_DEV + jnp.arange(DOC_DEV, dtype=jnp.int32)[None, :]
    shuffled = jnp.argsort(score_three, axis=-1).astype(jnp.int32)
    final_owner = jnp.take_along_axis(chosen_owner, shuffled, axis=1)
    local_draws = jax.random.randint(key_local, (3, DEVICES, DOC_DEV), 0, CL_DEV, dtype=jnp.int32)
    local_ids = jnp.min(local_draws, axis=0)
    slot_ids = final_owner * CL_DEV + local_ids
    return inverse[slot_ids.reshape(DOCS)]


def block_levels(stream_key, extent, pieces, smallest, high):
    gain, own = 1.0, jax.random.fold_in(stream_key, 6)
    for dim, shards_of in pieces:
        steps = jnp.exp(jax.random.uniform(jax.random.fold_in(own, dim), (shards_of,), jnp.float32, smallest / len(pieces), high / len(pieces)))
        gain = gain * jnp.repeat(steps, extent[dim] // shards_of).reshape([-1 if axis == dim else 1 for axis in range(len(extent))])
    return gain


def normal_values(key, shape, scale, reach, cuts=(), held_as=jnp.bfloat16):
    entries = jax.random.normal(key, shape, jnp.float32) * scale
    if len(cuts) > 0:
        entries = block_levels(key, shape, cuts, -0.22, 0.18) * entries
    return jnp.clip(entries, min=-reach, max=reach).astype(held_as)


def setup_inputs(seed: int = 0) -> dict:
    key_list = jax.random.split(jax.random.key(seed), 5)
    documents = normal_values(key_list[0], (DOCS, D), 1.0, 6.0, ((0, 32),))
    assigned = draw_assigned(jax.random.fold_in(key_list[4], 71), 0)
    centroids = normal_values(key_list[2], (CLUSTERS, D), 1.0, 6.0, ((0, 32),))
    owner_slot = draw_owner_slot(jax.random.fold_in(key_list[4], 71), 0)
    return dict(documents=documents, assigned=assigned, centroids=centroids, owner_slot=owner_slot)


def reference(documents, assigned, centroids, owner_slot):
    slot_ids = owner_slot[assigned]
    owner_ids = slot_ids // CL_DEV
    cent_sq = lax.optimization_barrier(jnp.sum(jnp.square(centroids.astype(jnp.float32)), axis=1))

    def block_sim(packed):
        doc_block, slot_block = packed
        doc_rows = doc_block.astype(jnp.float32)
        cent_rows = centroids[slot_block].astype(jnp.float32)
        cross_dot = lax.optimization_barrier(jnp.sum(doc_rows * cent_rows, axis=1))
        self_sq = lax.optimization_barrier(jnp.sum(doc_rows * doc_rows, axis=1))
        similar = cross_dot * lax.rsqrt(self_sq + 1.0) * lax.rsqrt(cent_sq[slot_block] + 1.0)
        return (similar, self_sq)
    similarity, self_sq = lax.map(block_sim, (documents.reshape(DEVICES, DOC_DEV, D), slot_ids.reshape(DEVICES, DOC_DEV)))
    similarity = similarity.reshape(DOCS)
    self_sq = self_sq.reshape(DOCS)
    counts = jax.ops.segment_sum(jnp.ones((DOCS,), jnp.float32), slot_ids, num_segments=CLUSTERS)
    totals = jax.ops.segment_sum(similarity, slot_ids, num_segments=CLUSTERS)
    squares = jax.ops.segment_sum(similarity * similarity, slot_ids, num_segments=CLUSTERS)
    cluster_stats = jnp.stack([counts, totals, squares])
    count_floor = jnp.maximum(counts, 1.0)
    mean_sim = totals / count_floor
    variance = jnp.maximum(squares / count_floor - mean_sim * mean_sim, 0.0)
    prototypicality = (mean_sim[slot_ids] - similarity) / jnp.sqrt(variance[slot_ids] + 1.0 / D)
    owner_grid = owner_ids.reshape(DEVICES, DOC_DEV)
    is_owner = (owner_grid[:, :, None] == jnp.arange(DEVICES, dtype=jnp.int32)[None, None, :]).astype(jnp.int32)
    rank_ids = lax.optimization_barrier(jnp.sum((jnp.cumsum(is_owner, axis=1) - 1) * is_owner, axis=2)).astype(jnp.int32)
    source_ids = jnp.arange(DEVICES, dtype=jnp.int32)[:, None]
    position = owner_grid * (DEVICES * CAP) + source_ids * CAP + rank_ids
    member_table = jnp.full((DEVICES * DEVICES * CAP,), DOCS, jnp.int32)
    member_table = member_table.at[position.reshape(-1)].set(jnp.arange(DOCS, dtype=jnp.int32))
    member_table = member_table.reshape(DEVICES, DEVICES * CAP)
    inverse_norm = lax.rsqrt(self_sq + 1.0)
    slot_count = DEVICES * CAP
    not_self = jnp.arange(slot_count, dtype=jnp.int32)[:, None] != jnp.arange(slot_count, dtype=jnp.int32)[None, :]

    def owner_redundancy(members):
        is_live = members < DOCS
        safe_ids = jnp.minimum(members, DOCS - 1)
        doc_rows = documents[safe_ids].astype(jnp.float32)
        gram_block = jnp.dot(doc_rows, doc_rows.T, precision=lax.Precision.HIGHEST)
        row_scale = jnp.where(is_live, inverse_norm[safe_ids], 0.0)
        cosine = gram_block * row_scale[:, None] * row_scale[None, :]
        cluster_tag = jnp.where(is_live, slot_ids[safe_ids], -1)
        same_cluster = (cluster_tag[:, None] == cluster_tag[None, :]) & is_live[:, None] & not_self
        return jnp.sqrt(jnp.float32(D)) * lax.optimization_barrier(jnp.max(jnp.where(same_cluster, cosine, 0.0), axis=1))
    redundant = lax.map(owner_redundancy, member_table)
    redundancy = jnp.zeros((DOCS,), jnp.float32).at[member_table.reshape(-1)].set(redundant.reshape(-1), mode='drop')
    return (prototypicality, redundancy, cluster_stats)
```

```python
import functools
import math

import jax
import jax.numpy as jnp
from jax import lax
from jax.experimental import pallas as pl
from jax.experimental.pallas import tpu as pltpu
from jax.sharding import PartitionSpec as P

F32 = jnp.float32
BF16 = jnp.bfloat16
HIGH = lax.Precision.HIGHEST
LANES = 128
SUB = 8


def round_up(value, unit):
    return -(-value // unit) * unit


def exclusive_or(left, right, extent):
    total = 0
    bit = 1
    while bit < extent:
        total = total + lax.rem(lax.rem(lax.div(left, bit), 2) + lax.rem(lax.div(right, bit), 2), 2) * bit
        bit *= 2
    return total


def iota(shape, dim):
    return lax.broadcasted_iota(jnp.int32, shape, dim)


def mm(left, right):
    return lax.dot_general(left, right, (((1,), (0,)), ((), ())), preferred_element_type=F32)


def mm_t(left, right):
    return lax.dot_general(left, right, (((1,), (1,)), ((), ())), preferred_element_type=F32)


def one_hot(condition):
    return jnp.where(condition, 1.0, 0.0).astype(BF16)


def kernel(
    dims,
    docs_ref,
    assigned_ref,
    cent_ref,
    table_ref,
    proto_ref,
    red_ref,
    stats_ref,
    send_buf,
    chunk_buf,
    code_send,
    code_recv,
    fwd_buf,
    rows_buf,
    tbl_send,
    tbl_recv,
    res_send,
    res_recv,
    pos_buf,
    tag_col,
    tag_row,
    inv_col,
    inv_row,
    sim_col,
    best_row,
    a_send,
    a_recv,
    m_send,
    m_recv,
    f_send,
    f_recv,
    t_send,
    t_recv,
    r_send,
    r_recv,
):
    R, C, K, Q = dims
    O = R * C
    CK = C * K
    L, D = docs_ref.shape
    S = cent_ref.shape[0]
    T = table_ref.shape[0]
    row_me = lax.axis_index("dp")
    col_me = lax.axis_index("cent")
    own = row_me * C + col_me

    def peer(q):
        step = lax.div(q, C)
        return step, exclusive_or(row_me, step, R), lax.rem(col_me + lax.rem(q, C), C)

    def where_is(r, c):
        return {"dp": r, "cent": c}

    def remote(src, dst, send, recv, r, c):
        return pltpu.make_async_remote_copy(
            src_ref=src,
            dst_ref=dst,
            send_sem=send,
            recv_sem=recv,
            device_id=where_is(r, c),
            device_id_type=pl.DeviceIdType.MESH,
        )

    barrier = pltpu.get_barrier_semaphore()

    def greet(q, carry):
        _, r, c = peer(q)
        pl.semaphore_signal(
            barrier, inc=1, device_id=where_is(r, c), device_id_type=pl.DeviceIdType.MESH
        )
        return carry

    lax.fori_loop(1, O, greet, 0)

    assigned = assigned_ref[...]
    high = lax.shift_right_logical(assigned, 7)
    low = jnp.bitwise_and(assigned, 127)
    table = table_ref[...]
    d0 = jnp.bitwise_and(table, 127)
    d1 = jnp.bitwise_and(lax.shift_right_logical(table, 7), 127)
    d2 = lax.shift_right_logical(table, 14)
    pick = one_hot(iota((T, L), 0) == high)

    def look(digit):
        return lax.dot_general(
            digit.astype(F32).astype(BF16), pick, (((0,), (0,)), ((), ())), preferred_element_type=F32
        )

    looked = look(d0) + 128.0 * look(d1) + 16384.0 * look(d2)
    slot = jnp.sum(jnp.where(iota((LANES, L), 0) == low, looked, 0.0), axis=0, keepdims=True)
    owner = jnp.floor((slot + 0.5) * (1.0 / S))
    local_id = slot - owner * S
    row = jnp.floor((owner + 0.5) * (1.0 / C))
    owner_i = owner.astype(jnp.int32)
    row_i = row.astype(jnp.int32)
    is_owner = jnp.where(iota((O, L), 0) == owner_i, 1.0, 0.0)
    is_row = jnp.where(iota((R, L), 0) == row_i, 1.0, 0.0)
    earlier = one_hot(iota((L, L), 0) < iota((L, L), 1))
    rank_owner = jnp.sum(mm(is_owner.astype(BF16), earlier) * is_owner, axis=0, keepdims=True)
    rank_row = jnp.sum(mm(is_row.astype(BF16), earlier) * is_row, axis=0, keepdims=True)
    position = (row * Q + rank_row).astype(jnp.int32)
    code = ((owner - row * C) * K + rank_owner + 1.0).astype(BF16)
    code8 = jnp.broadcast_to(code, (SUB, L))
    rank_i = rank_owner.astype(jnp.int32)
    pos_buf[...] = jnp.broadcast_to(position, (SUB, L))

    is_owner8 = lax.shift_right_logical(iota((O * SUB, L), 0), 3) == owner_i
    is_rank = one_hot(iota((LANES, L), 0) == rank_i)
    tag = local_id + 1.0
    tag_hi = jnp.floor(tag * (1.0 / 128.0))
    tag_lo = tag - tag_hi * 128.0
    tags = 128.0 * mm_t(jnp.where(is_owner8, tag_hi, 0.0).astype(BF16), is_rank) + mm_t(
        jnp.where(is_owner8, tag_lo, 0.0).astype(BF16), is_rank
    )
    tbl_send[...] = tags.reshape(O, SUB, LANES)

    pl.semaphore_wait(barrier, O - 1)

    def send_copy(t):
        r = exclusive_or(row_me, t, R)
        return (
            remote(send_buf.at[t], chunk_buf.at[t], a_send.at[t], a_recv.at[t], r, col_me),
            remote(code_send.at[t], code_recv.at[t], m_send.at[t], m_recv.at[t], r, col_me),
        )

    def bucket(t):
        r = exclusive_or(row_me, t, R)
        choose = one_hot(iota((Q, L), 0) + r * Q == pos_buf[0:1, :])
        return mm(choose, docs_ref[...]).astype(BF16), mm_t(code8, choose)

    def ship(t, carry):
        packed, codes = bucket(t)
        send_buf[t] = packed
        code_send[t] = codes
        for copy in send_copy(t):
            copy.start()
        return carry

    lax.fori_loop(1, R, ship, 0)
    packed, codes = bucket(0)
    chunk_buf[0] = packed
    code_recv[0] = codes

    def tbl_copy(q):
        t, r, c = peer(q)
        return remote(
            tbl_send.at[r * C + c], tbl_recv.at[t * C + col_me], t_send.at[q], t_recv.at[t * C + col_me], r, c
        )

    def tbl_arrival(q):
        t, r, c = peer(q)
        return remote(
            tbl_send.at[r * C + c], tbl_recv.at[t * C + c], t_send.at[q], t_recv.at[t * C + c], r, c
        )

    def start_tbl(q, carry):
        tbl_copy(q).start()
        return carry

    lax.fori_loop(1, O, start_tbl, 0)
    tbl_recv[col_me] = tbl_send[own]

    cent_sq = jnp.zeros((SUB, S), F32)
    ones = jnp.ones((SUB, 256), F32)

    squares = []
    for part in range(0, D, 256):
        block = cent_ref[:, part : part + 256].astype(F32)
        squares.append(block * block)
    while len(squares) > 1:
        squares = [a + b for a, b in zip(squares[::2], squares[1::2])] + (
            [squares[-1]] if len(squares) % 2 else []
        )
    cent_sq = lax.dot_general(
        ones, squares[0], (((1,), (1,)), ((), ())), precision=HIGH, preferred_element_type=F32
    )
    cent_inv = lax.rsqrt(cent_sq[0:1, :] + 1.0)

    def wait_tbl(q, carry):
        tbl_arrival(q).wait_recv()
        return carry

    lax.fori_loop(1, O, wait_tbl, 0)

    eye = iota((CK, CK), 0) == iota((CK, CK), 1)

    def spread(t, carry):
        column = jnp.zeros((CK, 1), F32)
        for c in range(C):
            line = tbl_recv[t * C + c][0:1, :]
            here = iota((CK, LANES), 0) - c * K == iota((CK, LANES), 1)
            here = here & (iota((CK, LANES), 1) < K)
            column = column + jnp.sum(jnp.where(here, line, 0.0), axis=1, keepdims=True)
        tag_col[t] = column
        flat = jnp.sum(jnp.where(eye, column, 0.0), axis=0, keepdims=True)
        tag_row[t] = jnp.where(flat > 0.0, flat, -1.0)
        return carry

    lax.fori_loop(0, R, spread, 0)

    stats_ref[...] = jnp.zeros(stats_ref.shape, F32)

    def fwd_copy(t, c):
        return remote(
            fwd_buf.at[t, c], rows_buf.at[t, col_me], f_send.at[t, c], f_recv.at[t, col_me], row_me, c
        )

    def fwd_arrival(t, c):
        return remote(fwd_buf.at[t, c], rows_buf.at[t, c], f_send.at[t, c], f_recv.at[t, c], row_me, c)

    def relay(t):
        codes = code_recv[t][0:1, :].astype(jnp.int32)
        choose = one_hot(iota((CK, Q), 0) + 1 == codes)
        fwd_buf[t] = mm(choose, chunk_buf[t]).astype(BF16).reshape(C, K, D)
        for d in range(1, C):
            fwd_copy(t, lax.rem(col_me + d, C)).start()
        rows_buf[t, col_me] = fwd_buf[t, col_me]

    def absorb(t):
        for d in range(1, C):
            fwd_arrival(t, lax.rem(col_me + d, C)).wait_recv()
        mine = rows_buf[t].reshape(CK, D)
        column = tag_col[t]
        line = tag_row[t]
        gram = mm_t(mine, mine)
        diag = jnp.where(eye, gram, 0.0)
        scale = lax.rsqrt(jnp.sum(diag, axis=1, keepdims=True) + 1.0)
        inv_col[t] = scale
        inv_row[t] = lax.rsqrt(jnp.sum(diag, axis=0, keepdims=True) + 1.0)
        member = iota((CK, S), 1).astype(F32) == column - 1.0
        cross = mm_t(mine, cent_ref[...]) * cent_inv
        similarity = jnp.sum(jnp.where(member, cross, 0.0), axis=1, keepdims=True) * scale
        sim_col[t] = similarity
        stats_ref[0:1, :] += jnp.sum(jnp.where(member, 1.0, 0.0), axis=0, keepdims=True)
        stats_ref[1:2, :] += jnp.sum(jnp.where(member, similarity, 0.0), axis=0, keepdims=True)
        stats_ref[2:3, :] += jnp.sum(
            jnp.where(member, similarity * similarity, 0.0), axis=0, keepdims=True
        )
        same = (column == line) & jnp.logical_not(eye)
        best = jnp.max(jnp.where(same, gram * scale, 0.0), axis=0, keepdims=True)

        def pair(u, best):
            other = rows_buf[u].reshape(CK, D)
            down = mm_t(other, mine)
            up = mm_t(mine, other)
            from_other = jnp.where(tag_col[u] == line, down * inv_col[u], 0.0)
            from_mine = jnp.where(column == tag_row[u], up * scale, 0.0)
            best_row[u] = jnp.maximum(best_row[u], jnp.max(from_mine, axis=0, keepdims=True))
            return jnp.maximum(best, jnp.max(from_other, axis=0, keepdims=True))

        best_row[t] = lax.fori_loop(0, t, pair, best)

    relay(0)

    def advance(t, carry):
        for copy in send_copy(t):
            copy.wait_recv()
        relay(t)
        absorb(t - 1)
        return carry

    lax.fori_loop(1, R, advance, 0)
    absorb(R - 1)

    floor = jnp.maximum(stats_ref[0:1, :], 1.0)
    mean = stats_ref[1:2, :] / floor
    variance = jnp.maximum(stats_ref[2:3, :] / floor - mean * mean, 0.0)
    spread_inv = 1.0 / jnp.sqrt(variance + 1.0 / D)

    def res_copy(q):
        t, r, c = peer(q)
        return remote(res_send.at[t * C + c], res_recv.at[own], r_send.at[q], r_recv.at[own], r, c)

    def res_arrival(q):
        t, r, c = peer(q)
        o = r * C + c
        return remote(res_send.at[t * C + c], res_recv.at[o], r_send.at[q], r_recv.at[o], r, c)

    half = LANES // 2

    def finish(t, carry):
        column = tag_col[t]
        member = iota((CK, S), 1).astype(F32) == column - 1.0
        centre = jnp.sum(jnp.where(member, mean, 0.0), axis=1, keepdims=True)
        width = jnp.sum(jnp.where(member, spread_inv, 0.0), axis=1, keepdims=True)
        proto = (centre - sim_col[t]) * width
        flat = best_row[t] * inv_row[t] * math.sqrt(D)
        redundant = jnp.sum(jnp.where(eye, flat, 0.0), axis=1, keepdims=True)
        lane = iota((CK, LANES), 1)
        rank = lax.rem(iota((CK, LANES), 0), K)
        lined = jnp.where(lane == rank, proto, 0.0) + jnp.where(lane == rank + half, redundant, 0.0)
        gather = lax.shift_right_logical(iota((C * SUB, CK), 0), 3) == lax.div(iota((C * SUB, CK), 1), K)
        packed = lax.dot_general(
            jnp.where(gather, 1.0, 0.0),
            lined,
            (((1,), (0,)), ((), ())),
            precision=HIGH,
            preferred_element_type=F32,
        )
        res_send[pl.ds(t * C, C)] = packed.reshape(C, SUB, LANES)
        return carry

    lax.fori_loop(0, R, finish, 0)

    def start_res(q, carry):
        res_copy(q).start()
        return carry

    lax.fori_loop(1, O, start_res, 0)
    res_recv[own] = res_send[col_me]

    def drain(t, carry):
        for copy in send_copy(t):
            copy.wait_send()
        return carry

    lax.fori_loop(1, R, drain, 0)

    def drain_fwd(t, carry):
        for d in range(1, C):
            fwd_copy(t, lax.rem(col_me + d, C)).wait_send()
        return carry

    lax.fori_loop(0, R, drain_fwd, 0)

    def drain_small(q, carry):
        tbl_copy(q).wait_send()
        res_copy(q).wait_send()
        return carry

    lax.fori_loop(1, O, drain_small, 0)

    def wait_res(q, carry):
        res_arrival(q).wait_recv()
        return carry

    lax.fori_loop(1, O, wait_res, 0)

    results = res_recv[...].reshape(O * SUB, LANES).T
    pick_owner = jnp.where(iota((O * SUB, L), 0) == owner_i * SUB, 1.0, 0.0)
    found = lax.dot_general(
        results, pick_owner, (((1,), (0,)), ((), ())), precision=HIGH, preferred_element_type=F32
    )
    sublane = iota((LANES, L), 0)
    proto_ref[...] = jnp.sum(jnp.where(sublane == rank_i, found, 0.0), axis=0, keepdims=True)
    red_ref[...] = jnp.sum(jnp.where(sublane == rank_i + half, found, 0.0), axis=0, keepdims=True)


def local(documents, assigned, centroids, owner_slot):
    L, D = documents.shape
    S = centroids.shape[0]
    R = lax.axis_size("dp")
    C = lax.axis_size("cent")
    O = R * C
    pair_cap = 2 * L // O
    row_cap = 5 * C * pair_cap // 8
    K = round_up(pair_cap, 16)
    Q = round_up(row_cap, 16)
    CK = C * K
    vmem = pl.BlockSpec(memory_space=pltpu.VMEM)
    dma = pltpu.SemaphoreType.DMA
    proto, red, stats = pl.pallas_call(
        functools.partial(kernel, (R, C, K, Q)),
        name="cluster_exchange",
        out_shape=(
            jax.ShapeDtypeStruct((1, L), F32),
            jax.ShapeDtypeStruct((1, L), F32),
            jax.ShapeDtypeStruct((3, S), F32),
        ),
        in_specs=[vmem] * 4,
        out_specs=(vmem, vmem, vmem),
        scratch_shapes=[
            pltpu.VMEM((R, Q, D), BF16),
            pltpu.VMEM((R, Q, D), BF16),
            pltpu.VMEM((R, SUB, Q), F32),
            pltpu.VMEM((R, SUB, Q), F32),
            pltpu.VMEM((R, C, K, D), BF16),
            pltpu.VMEM((R, C, K, D), BF16),
            pltpu.VMEM((O, SUB, LANES), F32),
            pltpu.VMEM((O, SUB, LANES), F32),
            pltpu.VMEM((O, SUB, LANES), F32),
            pltpu.VMEM((O, SUB, LANES), F32),
            pltpu.VMEM((SUB, L), jnp.int32),
            pltpu.VMEM((R, CK, 1), F32),
            pltpu.VMEM((R, 1, CK), F32),
            pltpu.VMEM((R, CK, 1), F32),
            pltpu.VMEM((R, 1, CK), F32),
            pltpu.VMEM((R, CK, 1), F32),
            pltpu.VMEM((R, 1, CK), F32),
            dma((R,)),
            dma((R,)),
            dma((R,)),
            dma((R,)),
            dma((R, C)),
            dma((R, C)),
            dma((O,)),
            dma((O,)),
            dma((O,)),
            dma((O,)),
        ],
        compiler_params=pltpu.CompilerParams(
            collective_id=0, has_side_effects=True, vmem_limit_bytes=62 * 1024 * 1024
        ),
    )(
        documents,
        assigned.reshape(1, L),
        centroids,
        owner_slot.reshape(-1, LANES),
    )
    return proto.reshape(L), red.reshape(L), stats


def solution(mesh):
    in_specs = (P(("dp", "cent"), None), P(("dp", "cent")), P(("dp", "cent"), None), P())
    out_specs = (P(("dp", "cent")), P(("dp", "cent")), P(None, ("dp", "cent")))
    return jax.shard_map(local, mesh=mesh, in_specs=in_specs, out_specs=out_specs, check_vma=False)
```

```python
import functools
import math

import jax
import jax.numpy as jnp
from jax import lax
from jax.experimental import pallas as pl
from jax.experimental.pallas import tpu as pltpu
from jax.sharding import PartitionSpec as P

F32 = jnp.float32
BF16 = jnp.bfloat16
HIGH = lax.Precision.HIGHEST
LANES = 128
SUB = 8


def round_up(value, unit):
    return -(-value // unit) * unit


def each(low, high, body):
    if high - low <= 8:
        for step in range(low, high):
            body(step)
    else:
        lax.fori_loop(low, high, lambda step, carry: (body(step), carry)[1], 0)


def iota(shape, dim):
    return lax.broadcasted_iota(jnp.int32, shape, dim)


def mm(left, right):
    return lax.dot_general(left, right, (((1,), (0,)), ((), ())), preferred_element_type=F32)


def mm_t(left, right):
    return lax.dot_general(left, right, (((1,), (1,)), ((), ())), preferred_element_type=F32)


def one_hot(condition):
    return jnp.where(condition, 1.0, 0.0).astype(BF16)


def kernel(
    dims,
    docs_ref,
    assigned_ref,
    cent_ref,
    table_ref,
    proto_ref,
    red_ref,
    stats_ref,
    send_buf,
    chunk_buf,
    code_send,
    code_recv,
    fwd_buf,
    rows_buf,
    tbl_send,
    tbl_recv,
    res_send,
    res_recv,
    tag_col,
    tag_row,
    inv_col,
    inv_row,
    sim_col,
    best_row,
    a_send,
    a_recv,
    m_send,
    m_recv,
    f_send,
    f_recv,
    t_send,
    t_recv,
    r_send,
    r_recv,
):
    R, C, K, Q = dims
    O = R * C
    CK = C * K
    L, D = docs_ref.shape
    S = cent_ref.shape[0]
    T = table_ref.shape[0]
    row_me = lax.axis_index("dp")
    col_me = lax.axis_index("cent")
    own = row_me * C + col_me

    bits = []
    while 2 ** len(bits) < R:
        bits.append(lax.rem(lax.div(row_me, 2 ** len(bits)), 2))
    col_of = [col_me] + [lax.rem(col_me + d, C) for d in range(1, C)]

    def row_of(t):
        total = 0
        for i, bit in enumerate(bits):
            if isinstance(t, int):
                total = total + (1 - bit if (t >> i) & 1 else bit) * 2**i
            else:
                total = total + lax.rem(bit + lax.div(t, 2**i), 2) * 2**i
        return total

    def all_peers(body):
        for d in range(1, C):
            body(0, row_me, d)

        def at_row(t):
            r = row_of(t)
            for d in range(C):
                body(t, r, d)

        each(1, R, at_row)

    def where_is(r, c):
        return {"dp": r, "cent": c}

    def remote(src, dst, send, recv, r, c):
        return pltpu.make_async_remote_copy(
            src_ref=src,
            dst_ref=dst,
            send_sem=send,
            recv_sem=recv,
            device_id=where_is(r, c),
            device_id_type=pl.DeviceIdType.MESH,
        )

    barrier = pltpu.get_barrier_semaphore()

    def greet(t, r, d):
        pl.semaphore_signal(
            barrier, inc=1, device_id=where_is(r, col_of[d]), device_id_type=pl.DeviceIdType.MESH
        )

    all_peers(greet)

    assigned = assigned_ref[...]
    high = lax.shift_right_logical(assigned, 7)
    low = jnp.bitwise_and(assigned, 127)
    table = table_ref[...]
    d0 = jnp.bitwise_and(table, 127)
    d1 = jnp.bitwise_and(lax.shift_right_logical(table, 7), 127)
    d2 = lax.shift_right_logical(table, 14)
    pick = one_hot(iota((T, L), 0) == high)

    def look(digit):
        return lax.dot_general(
            digit.astype(F32).astype(BF16), pick, (((0,), (0,)), ((), ())), preferred_element_type=F32
        )

    looked = look(d0) + 128.0 * look(d1) + 16384.0 * look(d2)
    slot = jnp.sum(jnp.where(iota((LANES, L), 0) == low, looked, 0.0), axis=0, keepdims=True)
    owner = jnp.floor((slot + 0.5) * (1.0 / S))
    local_id = slot - owner * S
    row = jnp.floor((owner + 0.5) * (1.0 / C))
    owner_i = owner.astype(jnp.int32)
    row_i = row.astype(jnp.int32)
    is_owner = jnp.where(iota((O, L), 0) == owner_i, 1.0, 0.0)
    is_row = jnp.where(iota((R, L), 0) == row_i, 1.0, 0.0)
    earlier = one_hot(iota((L, L), 0) < iota((L, L), 1))
    rank_owner = jnp.sum(mm(is_owner.astype(BF16), earlier) * is_owner, axis=0, keepdims=True)
    rank_row = jnp.sum(mm(is_row.astype(BF16), earlier) * is_row, axis=0, keepdims=True)
    position = jnp.bitwise_xor(row_i, row_me) * Q + rank_row.astype(jnp.int32)
    code = ((owner - row * C) * K + rank_owner + 1.0).astype(BF16)
    code8 = jnp.broadcast_to(code, (SUB, L))
    rank_i = rank_owner.astype(jnp.int32)
    docs = docs_ref[...]

    is_owner8 = lax.shift_right_logical(iota((O * SUB, L), 0), 3) == owner_i
    is_rank = one_hot(iota((LANES, L), 0) == rank_i)
    tag = local_id + 1.0
    tag_hi = jnp.floor(tag * (1.0 / 128.0))
    tag_lo = tag - tag_hi * 128.0
    tags = 128.0 * mm_t(jnp.where(is_owner8, tag_hi, 0.0).astype(BF16), is_rank) + mm_t(
        jnp.where(is_owner8, tag_lo, 0.0).astype(BF16), is_rank
    )
    tbl_send[...] = tags.reshape(O, SUB, LANES)

    pl.semaphore_wait(barrier, O - 1)

    def tbl_copy(t, r, d):
        return remote(
            tbl_send.at[r * C + col_of[d]],
            tbl_recv.at[t * C + col_me],
            t_send.at[t * C + d],
            t_recv.at[t * C + col_me],
            r,
            col_of[d],
        )

    def tbl_arrival(t, r, d):
        return remote(
            tbl_send.at[r * C + col_of[d]],
            tbl_recv.at[t * C + col_of[d]],
            t_send.at[t * C + d],
            t_recv.at[t * C + col_of[d]],
            r,
            col_of[d],
        )

    all_peers(lambda t, r, d: tbl_copy(t, r, d).start())
    tbl_recv[col_me] = tbl_send[own]

    def row_copy(t, r):
        return remote(send_buf.at[t], chunk_buf.at[t], a_send.at[t], a_recv.at[t], r, col_me)

    def code_copy(t, r):
        return remote(code_send.at[t], code_recv.at[t], m_send.at[t], m_recv.at[t], r, col_me)

    def mark(t):
        code_send[t] = mm_t(code8, one_hot(iota((Q, L), 0) + t * Q == position))

    each(0, R, mark)
    each(1, R, lambda t: code_copy(t, row_of(t)).start())
    code_recv[0] = code_send[0]

    group = max(1, R // 2)
    for first in range(0, R, group):
        choose = one_hot(iota((group * Q, L), 0) + first * Q == position)
        send_buf[first : first + group] = mm(choose, docs).astype(BF16).reshape(group, Q, D)
        each(max(first, 1), first + group, lambda t: row_copy(t, row_of(t)).start())
    chunk_buf[0] = send_buf[0]

    def fwd_copy(t, c):
        return remote(
            fwd_buf.at[t, c], rows_buf.at[t, col_me], f_send.at[t, c], f_recv.at[t, col_me], row_me, c
        )

    def fwd_arrival(t, c):
        return remote(fwd_buf.at[t, c], rows_buf.at[t, c], f_send.at[t, c], f_recv.at[t, c], row_me, c)

    def relay(t):
        codes = code_recv[t][0:1, :].astype(jnp.int32)
        choose = one_hot(iota((CK, Q), 0) + 1 == codes)
        fwd_buf[t] = mm(choose, chunk_buf[t]).astype(BF16).reshape(C, K, D)
        for d in range(1, C):
            fwd_copy(t, col_of[d]).start()
        rows_buf[t, col_me] = fwd_buf[t, col_me]

    relay(0)

    ones = jnp.ones((SUB, 256), F32)

    squares = []
    for part in range(0, D, 256):
        block = cent_ref[:, part : part + 256].astype(F32)
        squares.append(block * block)
    while len(squares) > 1:
        squares = [a + b for a, b in zip(squares[::2], squares[1::2])] + (
            [squares[-1]] if len(squares) % 2 else []
        )
    cent_sq = lax.dot_general(
        ones, squares[0], (((1,), (1,)), ((), ())), precision=HIGH, preferred_element_type=F32
    )
    cent_inv = lax.rsqrt(cent_sq[0:1, :] + 1.0)

    all_peers(lambda t, r, d: tbl_arrival(t, r, d).wait_recv())

    eye = iota((CK, CK), 0) == iota((CK, CK), 1)

    def spread(t, carry):
        column = jnp.zeros((CK, 1), F32)
        for c in range(C):
            line = tbl_recv[t * C + c][0:1, :]
            here = iota((CK, LANES), 0) - c * K == iota((CK, LANES), 1)
            here = here & (iota((CK, LANES), 1) < K)
            column = column + jnp.sum(jnp.where(here, line, 0.0), axis=1, keepdims=True)
        tag_col[t] = column
        flat = jnp.sum(jnp.where(eye, column, 0.0), axis=0, keepdims=True)
        tag_row[t] = jnp.where(flat > 0.0, flat, -1.0)
        return carry

    lax.fori_loop(0, R, spread, 0)

    stats_ref[...] = jnp.zeros(stats_ref.shape, F32)

    def absorb(t):
        for d in range(1, C):
            fwd_arrival(t, col_of[d]).wait_recv()
        mine = rows_buf[t].reshape(CK, D)
        column = tag_col[t]
        line = tag_row[t]
        gram = mm_t(mine, mine)
        diag = jnp.where(eye, gram, 0.0)
        scale = lax.rsqrt(jnp.sum(diag, axis=1, keepdims=True) + 1.0)
        inv_col[t] = scale
        inv_row[t] = lax.rsqrt(jnp.sum(diag, axis=0, keepdims=True) + 1.0)
        member = iota((CK, S), 1).astype(F32) == column - 1.0
        cross = mm_t(mine, cent_ref[...]) * cent_inv
        similarity = jnp.sum(jnp.where(member, cross, 0.0), axis=1, keepdims=True) * scale
        sim_col[t] = similarity
        stats_ref[0:1, :] += jnp.sum(jnp.where(member, 1.0, 0.0), axis=0, keepdims=True)
        stats_ref[1:2, :] += jnp.sum(jnp.where(member, similarity, 0.0), axis=0, keepdims=True)
        stats_ref[2:3, :] += jnp.sum(
            jnp.where(member, similarity * similarity, 0.0), axis=0, keepdims=True
        )
        same = (column == line) & jnp.logical_not(eye)
        best = jnp.max(jnp.where(same, gram * scale, 0.0), axis=0, keepdims=True)

        def pair(u, best):
            other = rows_buf[u].reshape(CK, D)
            down = mm_t(other, mine)
            up = mm_t(mine, other)
            from_other = jnp.where(tag_col[u] == line, down * inv_col[u], 0.0)
            from_mine = jnp.where(column == tag_row[u], up * scale, 0.0)
            best_row[u] = jnp.maximum(best_row[u], jnp.max(from_mine, axis=0, keepdims=True))
            return jnp.maximum(best, jnp.max(from_other, axis=0, keepdims=True))

        best_row[t] = lax.fori_loop(0, t, pair, best)

    def advance(t, carry):
        code_copy(t, row_of(R - 1)).wait_recv()
        row_copy(t, row_of(R - 1)).wait_recv()
        relay(t)
        absorb(t - 1)
        return carry

    lax.fori_loop(1, R, advance, 0)
    absorb(R - 1)

    floor = jnp.maximum(stats_ref[0:1, :], 1.0)
    mean = stats_ref[1:2, :] / floor
    variance = jnp.maximum(stats_ref[2:3, :] / floor - mean * mean, 0.0)
    spread_inv = 1.0 / jnp.sqrt(variance + 1.0 / D)

    def res_copy(t, r, d):
        return remote(
            res_send.at[t * C + col_of[d]],
            res_recv.at[own],
            r_send.at[t * C + d],
            r_recv.at[own],
            r,
            col_of[d],
        )

    def res_arrival(t, r, d):
        o = r * C + col_of[d]
        return remote(
            res_send.at[t * C + col_of[d]], res_recv.at[o], r_send.at[t * C + d], r_recv.at[o], r, col_of[d]
        )

    half = LANES // 2

    def finish(t, carry):
        column = tag_col[t]
        member = iota((CK, S), 1).astype(F32) == column - 1.0
        centre = jnp.sum(jnp.where(member, mean, 0.0), axis=1, keepdims=True)
        width = jnp.sum(jnp.where(member, spread_inv, 0.0), axis=1, keepdims=True)
        proto = (centre - sim_col[t]) * width
        flat = best_row[t] * inv_row[t] * math.sqrt(D)
        redundant = jnp.sum(jnp.where(eye, flat, 0.0), axis=1, keepdims=True)
        lane = iota((CK, LANES), 1)
        rank = lax.rem(iota((CK, LANES), 0), K)
        lined = jnp.where(lane == rank, proto, 0.0) + jnp.where(lane == rank + half, redundant, 0.0)
        gather = lax.shift_right_logical(iota((C * SUB, CK), 0), 3) == lax.div(iota((C * SUB, CK), 1), K)
        packed = lax.dot_general(
            jnp.where(gather, 1.0, 0.0),
            lined,
            (((1,), (0,)), ((), ())),
            precision=HIGH,
            preferred_element_type=F32,
        )
        res_send[pl.ds(t * C, C)] = packed.reshape(C, SUB, LANES)
        return carry

    lax.fori_loop(0, R, finish, 0)

    all_peers(lambda t, r, d: res_copy(t, r, d).start())
    res_recv[own] = res_send[col_me]

    def drain(t):
        code_copy(t, row_of(t)).wait_send()
        row_copy(t, row_of(t)).wait_send()

    each(1, R, drain)

    def drain_fwd(t):
        for d in range(1, C):
            fwd_copy(t, col_of[d]).wait_send()

    each(0, R, drain_fwd)

    def drain_small(t, r, d):
        tbl_copy(t, r, d).wait_send()
        res_copy(t, r, d).wait_send()

    all_peers(drain_small)
    all_peers(lambda t, r, d: res_arrival(t, r, d).wait_recv())

    results = res_recv[...].reshape(O * SUB, LANES).T
    pick_owner = jnp.where(iota((O * SUB, L), 0) == owner_i * SUB, 1.0, 0.0)
    found = lax.dot_general(
        results, pick_owner, (((1,), (0,)), ((), ())), precision=HIGH, preferred_element_type=F32
    )
    sublane = iota((LANES, L), 0)
    proto_ref[...] = jnp.sum(jnp.where(sublane == rank_i, found, 0.0), axis=0, keepdims=True)
    red_ref[...] = jnp.sum(jnp.where(sublane == rank_i + half, found, 0.0), axis=0, keepdims=True)


def local(documents, assigned, centroids, owner_slot):
    L, D = documents.shape
    S = centroids.shape[0]
    R = lax.axis_size("dp")
    C = lax.axis_size("cent")
    O = R * C
    pair_cap = 2 * L // O
    row_cap = 5 * C * pair_cap // 8
    K = round_up(pair_cap, 16)
    Q = round_up(row_cap, 16)
    CK = C * K
    vmem = pl.BlockSpec(memory_space=pltpu.VMEM)
    dma = pltpu.SemaphoreType.DMA
    proto, red, stats = pl.pallas_call(
        functools.partial(kernel, (R, C, K, Q)),
        name="cluster_exchange",
        out_shape=(
            jax.ShapeDtypeStruct((1, L), F32),
            jax.ShapeDtypeStruct((1, L), F32),
            jax.ShapeDtypeStruct((3, S), F32),
        ),
        in_specs=[vmem] * 4,
        out_specs=(vmem, vmem, vmem),
        scratch_shapes=[
            pltpu.VMEM((R, Q, D), BF16),
            pltpu.VMEM((R, Q, D), BF16),
            pltpu.VMEM((R, SUB, Q), F32),
            pltpu.VMEM((R, SUB, Q), F32),
            pltpu.VMEM((R, C, K, D), BF16),
            pltpu.VMEM((R, C, K, D), BF16),
            pltpu.VMEM((O, SUB, LANES), F32),
            pltpu.VMEM((O, SUB, LANES), F32),
            pltpu.VMEM((O, SUB, LANES), F32),
            pltpu.VMEM((O, SUB, LANES), F32),
            pltpu.VMEM((R, CK, 1), F32),
            pltpu.VMEM((R, 1, CK), F32),
            pltpu.VMEM((R, CK, 1), F32),
            pltpu.VMEM((R, 1, CK), F32),
            pltpu.VMEM((R, CK, 1), F32),
            pltpu.VMEM((R, 1, CK), F32),
            dma((R,)),
            dma((R,)),
            dma((R,)),
            dma((R,)),
            dma((R, C)),
            dma((R, C)),
            dma((O,)),
            dma((O,)),
            dma((O,)),
            dma((O,)),
        ],
        compiler_params=pltpu.CompilerParams(
            collective_id=0, has_side_effects=True, vmem_limit_bytes=62 * 1024 * 1024
        ),
    )(
        documents,
        assigned.reshape(1, L),
        centroids,
        owner_slot.reshape(-1, LANES),
    )
    return proto.reshape(L), red.reshape(L), stats


def solution(mesh):
    in_specs = (P(("dp", "cent"), None), P(("dp", "cent")), P(("dp", "cent"), None), P())
    out_specs = (P(("dp", "cent")), P(("dp", "cent")), P(None, ("dp", "cent")))
    return jax.shard_map(local, mesh=mesh, in_specs=in_specs, out_specs=out_specs, check_vma=False)
```

```python
import functools
import math

import jax
import jax.numpy as jnp
from jax import lax
from jax.experimental import pallas as pl
from jax.experimental.pallas import tpu as pltpu
from jax.sharding import PartitionSpec as P

F32 = jnp.float32
BF16 = jnp.bfloat16
HIGH = lax.Precision.HIGHEST
LANES = 128
SUB = 8


def round_up(value, unit):
    return -(-value // unit) * unit


def each(low, high, body):
    if high - low <= 8:
        for step in range(low, high):
            body(step)
    else:
        lax.fori_loop(low, high, lambda step, carry: (body(step), carry)[1], 0)


def iota(shape, dim):
    return lax.broadcasted_iota(jnp.int32, shape, dim)


def mm(left, right):
    return lax.dot_general(left, right, (((1,), (0,)), ((), ())), preferred_element_type=F32)


def mm_t(left, right):
    return lax.dot_general(left, right, (((1,), (1,)), ((), ())), preferred_element_type=F32)


def one_hot(condition):
    return jnp.where(condition, 1.0, 0.0).astype(BF16)


def kernel(
    dims,
    docs_ref,
    assigned_ref,
    cent_ref,
    table_ref,
    out_ref,
    send_buf,
    chunk_buf,
    code_send,
    code_recv,
    fwd_buf,
    rows_buf,
    tbl_send,
    tbl_recv,
    res_send,
    res_recv,
    tag_col,
    tag_row,
    inv_col,
    inv_row,
    sim_col,
    best_row,
    a_send,
    a_recv,
    m_send,
    m_recv,
    f_send,
    f_recv,
    t_send,
    t_recv,
    r_send,
    r_recv,
    stats_ref,
):
    R, C, K, Q = dims
    O = R * C
    CK = C * K
    L, D = docs_ref.shape
    S = cent_ref.shape[0]
    T = table_ref.shape[0]
    row_me = lax.axis_index("dp")
    col_me = lax.axis_index("cent")
    own = row_me * C + col_me

    bits = []
    while 2 ** len(bits) < R:
        bits.append(lax.rem(lax.div(row_me, 2 ** len(bits)), 2))
    col_of = [col_me] + [lax.rem(col_me + d, C) for d in range(1, C)]

    def row_of(t):
        total = 0
        for i, bit in enumerate(bits):
            if isinstance(t, int):
                total = total + (1 - bit if (t >> i) & 1 else bit) * 2**i
            else:
                total = total + lax.rem(bit + lax.div(t, 2**i), 2) * 2**i
        return total

    def all_peers(body):
        for d in range(1, C):
            body(0, row_me, d)

        def at_row(t):
            r = row_of(t)
            for d in range(C):
                body(t, r, d)

        each(1, R, at_row)

    def where_is(r, c):
        return {"dp": r, "cent": c}

    def remote(src, dst, send, recv, r, c):
        return pltpu.make_async_remote_copy(
            src_ref=src,
            dst_ref=dst,
            send_sem=send,
            recv_sem=recv,
            device_id=where_is(r, c),
            device_id_type=pl.DeviceIdType.MESH,
        )

    barrier = pltpu.get_barrier_semaphore()

    def greet(t, r, d):
        pl.semaphore_signal(
            barrier, inc=1, device_id=where_is(r, col_of[d]), device_id_type=pl.DeviceIdType.MESH
        )

    all_peers(greet)

    assigned = assigned_ref[...]
    high = lax.shift_right_logical(assigned, 7)
    low = jnp.bitwise_and(assigned, 127)
    table = table_ref[...]
    d0 = jnp.bitwise_and(table, 127)
    d1 = jnp.bitwise_and(lax.shift_right_logical(table, 7), 127)
    d2 = lax.shift_right_logical(table, 14)
    pick = one_hot(iota((T, L), 0) == high)

    def look(digit):
        return lax.dot_general(
            digit.astype(F32).astype(BF16), pick, (((0,), (0,)), ((), ())), preferred_element_type=F32
        )

    looked = look(d0) + 128.0 * look(d1) + 16384.0 * look(d2)
    slot = jnp.sum(jnp.where(iota((LANES, L), 0) == low, looked, 0.0), axis=0, keepdims=True)
    owner = jnp.floor((slot + 0.5) * (1.0 / S))
    local_id = slot - owner * S
    row = jnp.floor((owner + 0.5) * (1.0 / C))
    owner_i = owner.astype(jnp.int32)
    row_i = row.astype(jnp.int32)
    is_owner = jnp.where(iota((O, L), 0) == owner_i, 1.0, 0.0)
    is_row = jnp.where(iota((R, L), 0) == row_i, 1.0, 0.0)
    earlier = one_hot(iota((L, L), 0) < iota((L, L), 1))
    rank_owner = jnp.sum(mm(is_owner.astype(BF16), earlier) * is_owner, axis=0, keepdims=True)
    rank_row = jnp.sum(mm(is_row.astype(BF16), earlier) * is_row, axis=0, keepdims=True)
    position = jnp.bitwise_xor(row_i, row_me) * Q + rank_row.astype(jnp.int32)
    code = ((owner - row * C) * K + rank_owner + 1.0).astype(BF16)
    code8 = jnp.broadcast_to(code, (SUB, L))
    rank_i = rank_owner.astype(jnp.int32)
    docs = docs_ref[...]

    is_owner8 = lax.shift_right_logical(iota((O * SUB, L), 0), 3) == owner_i
    is_rank = one_hot(iota((LANES, L), 0) == rank_i)
    tag = local_id + 1.0
    tag_hi = jnp.floor(tag * (1.0 / 128.0))
    tag_lo = tag - tag_hi * 128.0
    tags = 128.0 * mm_t(jnp.where(is_owner8, tag_hi, 0.0).astype(BF16), is_rank) + mm_t(
        jnp.where(is_owner8, tag_lo, 0.0).astype(BF16), is_rank
    )
    tbl_send[...] = tags.reshape(O, SUB, LANES)

    pl.semaphore_wait(barrier, O - 1)

    def tbl_copy(t, r, d):
        return remote(
            tbl_send.at[r * C + col_of[d]],
            tbl_recv.at[t * C + col_me],
            t_send.at[t * C + d],
            t_recv.at[t * C + col_me],
            r,
            col_of[d],
        )

    def tbl_arrival(t, r, d):
        return remote(
            tbl_send.at[r * C + col_of[d]],
            tbl_recv.at[t * C + col_of[d]],
            t_send.at[t * C + d],
            t_recv.at[t * C + col_of[d]],
            r,
            col_of[d],
        )

    all_peers(lambda t, r, d: tbl_copy(t, r, d).start())
    tbl_recv[col_me] = tbl_send[own]

    def row_copy(t, r):
        return remote(send_buf.at[t], chunk_buf.at[t], a_send.at[t], a_recv.at[t], r, col_me)

    def code_copy(t, r):
        return remote(code_send.at[t], code_recv.at[t], m_send.at[t], m_recv.at[t], r, col_me)

    def mark(t):
        code_send[t] = mm_t(code8, one_hot(iota((Q, L), 0) + t * Q == position))

    each(0, R, mark)
    each(1, R, lambda t: code_copy(t, row_of(t)).start())
    code_recv[0] = code_send[0]

    group = max(1, R // 2)
    for first in range(0, R, group):
        choose = one_hot(iota((group * Q, L), 0) + first * Q == position)
        send_buf[first : first + group] = mm(choose, docs).astype(BF16).reshape(group, Q, D)
        each(max(first, 1), first + group, lambda t: row_copy(t, row_of(t)).start())
    chunk_buf[0] = send_buf[0]

    def fwd_copy(t, c):
        return remote(
            fwd_buf.at[t, c], rows_buf.at[t, col_me], f_send.at[t, c], f_recv.at[t, col_me], row_me, c
        )

    def fwd_arrival(t, c):
        return remote(fwd_buf.at[t, c], rows_buf.at[t, c], f_send.at[t, c], f_recv.at[t, c], row_me, c)

    def relay(t):
        codes = code_recv[t][0:1, :].astype(jnp.int32)
        choose = one_hot(iota((CK, Q), 0) + 1 == codes)
        fwd_buf[t] = mm(choose, chunk_buf[t]).astype(BF16).reshape(C, K, D)
        for d in range(1, C):
            fwd_copy(t, col_of[d]).start()
        rows_buf[t, col_me] = fwd_buf[t, col_me]

    relay(0)

    ones = jnp.ones((SUB, 256), F32)

    squares = []
    for part in range(0, D, 256):
        block = cent_ref[:, part : part + 256].astype(F32)
        squares.append(block * block)
    while len(squares) > 1:
        squares = [a + b for a, b in zip(squares[::2], squares[1::2])] + (
            [squares[-1]] if len(squares) % 2 else []
        )
    cent_sq = lax.dot_general(
        ones, squares[0], (((1,), (1,)), ((), ())), precision=HIGH, preferred_element_type=F32
    )
    cent_inv = lax.rsqrt(cent_sq[0:1, :] + 1.0)

    all_peers(lambda t, r, d: tbl_arrival(t, r, d).wait_recv())

    eye = iota((CK, CK), 0) == iota((CK, CK), 1)

    def spread(t):
        column = jnp.zeros((CK, 1), F32)
        for c in range(C):
            line = tbl_recv[t * C + c][0:1, :]
            here = iota((CK, LANES), 0) - c * K == iota((CK, LANES), 1)
            here = here & (iota((CK, LANES), 1) < K)
            column = column + jnp.sum(jnp.where(here, line, 0.0), axis=1, keepdims=True)
        tag_col[t] = column
        flat = jnp.sum(jnp.where(eye, column, 0.0), axis=0, keepdims=True)
        tag_row[t] = jnp.where(flat > 0.0, flat, -1.0)

    each(0, R, spread)

    stats_ref[...] = jnp.zeros(stats_ref.shape, F32)

    def absorb(t):
        for d in range(1, C):
            fwd_arrival(t, col_of[d]).wait_recv()
        mine = rows_buf[t].reshape(CK, D)
        column = tag_col[t]
        line = tag_row[t]
        gram = mm_t(mine, mine)
        diag = jnp.where(eye, gram, 0.0)
        scale = lax.rsqrt(jnp.sum(diag, axis=1, keepdims=True) + 1.0)
        inv_col[t] = scale
        inv_row[t] = lax.rsqrt(jnp.sum(diag, axis=0, keepdims=True) + 1.0)
        member = iota((CK, S), 1).astype(F32) == column - 1.0
        cross = mm_t(mine, cent_ref[...]) * cent_inv
        similarity = jnp.sum(jnp.where(member, cross, 0.0), axis=1, keepdims=True) * scale
        sim_col[t] = similarity
        stats_ref[0:1, :] += jnp.sum(jnp.where(member, 1.0, 0.0), axis=0, keepdims=True)
        stats_ref[1:2, :] += jnp.sum(jnp.where(member, similarity, 0.0), axis=0, keepdims=True)
        stats_ref[2:3, :] += jnp.sum(
            jnp.where(member, similarity * similarity, 0.0), axis=0, keepdims=True
        )
        same = (column == line) & jnp.logical_not(eye)
        best = jnp.max(jnp.where(same, gram * scale, 0.0), axis=0, keepdims=True)

        def pair(u, best):
            other = rows_buf[u].reshape(CK, D)
            down = mm_t(other, mine)
            up = mm_t(mine, other)
            from_other = jnp.where(tag_col[u] == line, down * inv_col[u], 0.0)
            from_mine = jnp.where(column == tag_row[u], up * scale, 0.0)
            best_row[u] = jnp.maximum(best_row[u], jnp.max(from_mine, axis=0, keepdims=True))
            return jnp.maximum(best, jnp.max(from_other, axis=0, keepdims=True))

        best_row[t] = lax.fori_loop(0, t, pair, best)

    def advance(t, carry):
        code_copy(t, row_of(R - 1)).wait_recv()
        row_copy(t, row_of(R - 1)).wait_recv()
        relay(t)
        absorb(t - 1)
        return carry

    lax.fori_loop(1, R, advance, 0)
    absorb(R - 1)

    floor = jnp.maximum(stats_ref[0:1, :], 1.0)
    mean = stats_ref[1:2, :] / floor
    variance = jnp.maximum(stats_ref[2:3, :] / floor - mean * mean, 0.0)
    out_ref[2:5, :S] = stats_ref[...]
    spread_inv = 1.0 / jnp.sqrt(variance + 1.0 / D)

    def res_copy(t, r, d):
        return remote(
            res_send.at[t * C + col_of[d]],
            res_recv.at[own],
            r_send.at[t * C + d],
            r_recv.at[own],
            r,
            col_of[d],
        )

    def res_arrival(t, r, d):
        o = r * C + col_of[d]
        return remote(
            res_send.at[t * C + col_of[d]], res_recv.at[o], r_send.at[t * C + d], r_recv.at[o], r, col_of[d]
        )

    half = LANES // 2

    def finish(t):
        column = tag_col[t]
        member = iota((CK, S), 1).astype(F32) == column - 1.0
        centre = jnp.sum(jnp.where(member, mean, 0.0), axis=1, keepdims=True)
        width = jnp.sum(jnp.where(member, spread_inv, 0.0), axis=1, keepdims=True)
        proto = (centre - sim_col[t]) * width
        flat = best_row[t] * inv_row[t] * math.sqrt(D)
        redundant = jnp.sum(jnp.where(eye, flat, 0.0), axis=1, keepdims=True)
        lane = iota((CK, LANES), 1)
        rank = lax.rem(iota((CK, LANES), 0), K)
        lined = jnp.where(lane == rank, proto, 0.0) + jnp.where(lane == rank + half, redundant, 0.0)
        gather = lax.shift_right_logical(iota((C * SUB, CK), 0), 3) == lax.div(iota((C * SUB, CK), 1), K)
        packed = lax.dot_general(
            jnp.where(gather, 1.0, 0.0),
            lined,
            (((1,), (0,)), ((), ())),
            precision=HIGH,
            preferred_element_type=F32,
        )
        res_send[pl.ds(t * C, C)] = packed.reshape(C, SUB, LANES)

    def deliver(t):
        finish(t)
        r = row_of(t)
        for d in range(C):
            res_copy(t, r, d).start()

    each(1, R, deliver)
    finish(0)
    for d in range(1, C):
        res_copy(0, row_me, d).start()
    res_recv[own] = res_send[col_me]

    def drain(t):
        code_copy(t, row_of(t)).wait_send()
        row_copy(t, row_of(t)).wait_send()

    each(1, R, drain)

    def drain_fwd(t):
        for d in range(1, C):
            fwd_copy(t, col_of[d]).wait_send()

    each(0, R, drain_fwd)

    def drain_small(t, r, d):
        tbl_copy(t, r, d).wait_send()
        res_copy(t, r, d).wait_send()

    all_peers(drain_small)
    all_peers(lambda t, r, d: res_arrival(t, r, d).wait_recv())

    results = res_recv[...].reshape(O * SUB, LANES).T
    pick_owner = jnp.where(iota((O * SUB, L), 0) == owner_i * SUB, 1.0, 0.0)
    found = lax.dot_general(
        results, pick_owner, (((1,), (0,)), ((), ())), precision=HIGH, preferred_element_type=F32
    )
    sublane = iota((LANES, L), 0)
    out_ref[0:1, :L] = jnp.sum(jnp.where(sublane == rank_i, found, 0.0), axis=0, keepdims=True)
    out_ref[1:2, :L] = jnp.sum(jnp.where(sublane == rank_i + half, found, 0.0), axis=0, keepdims=True)


def local(documents, assigned, centroids, owner_slot):
    L, D = documents.shape
    S = centroids.shape[0]
    R = lax.axis_size("dp")
    C = lax.axis_size("cent")
    O = R * C
    pair_cap = 2 * L // O
    row_cap = 5 * C * pair_cap // 8
    K = round_up(pair_cap, 16)
    Q = round_up(row_cap, 16)
    CK = C * K
    vmem = pl.BlockSpec(memory_space=pltpu.VMEM)
    dma = pltpu.SemaphoreType.DMA
    packed = pl.pallas_call(
        functools.partial(kernel, (R, C, K, Q)),
        name="cluster_exchange",
        out_shape=jax.ShapeDtypeStruct((SUB, max(L, S)), F32),
        in_specs=[vmem] * 4,
        out_specs=vmem,
        scratch_shapes=[
            pltpu.VMEM((R, Q, D), BF16),
            pltpu.VMEM((R, Q, D), BF16),
            pltpu.VMEM((R, SUB, Q), F32),
            pltpu.VMEM((R, SUB, Q), F32),
            pltpu.VMEM((R, C, K, D), BF16),
            pltpu.VMEM((R, C, K, D), BF16),
            pltpu.VMEM((O, SUB, LANES), F32),
            pltpu.VMEM((O, SUB, LANES), F32),
            pltpu.VMEM((O, SUB, LANES), F32),
            pltpu.VMEM((O, SUB, LANES), F32),
            pltpu.VMEM((R, CK, 1), F32),
            pltpu.VMEM((R, 1, CK), F32),
            pltpu.VMEM((R, CK, 1), F32),
            pltpu.VMEM((R, 1, CK), F32),
            pltpu.VMEM((R, CK, 1), F32),
            pltpu.VMEM((R, 1, CK), F32),
            dma((R,)),
            dma((R,)),
            dma((R,)),
            dma((R,)),
            dma((R, C)),
            dma((R, C)),
            dma((O,)),
            dma((O,)),
            dma((O,)),
            dma((O,)),
            pltpu.VMEM((3, S), F32),
        ],
        compiler_params=pltpu.CompilerParams(
            collective_id=0, has_side_effects=True, vmem_limit_bytes=62 * 1024 * 1024
        ),
    )(
        documents,
        assigned.reshape(1, L),
        centroids,
        owner_slot.reshape(-1, LANES),
    )
    return packed[0, :L], packed[1, :L], packed[2:5, :S]


def solution(mesh):
    in_specs = (P(("dp", "cent"), None), P(("dp", "cent")), P(("dp", "cent"), None), P())
    out_specs = (P(("dp", "cent")), P(("dp", "cent")), P(None, ("dp", "cent")))
    return jax.shard_map(local, mesh=mesh, in_specs=in_specs, out_specs=out_specs, check_vma=False)
```
